32 devices in a mesh: gx: 4 (over x, core), gy: 8 (over z, y).
Axes of the slice: x: 2, y: 2, z: 4, core: 2. Of those that a mesh axis runs over, the one named last changes fastest.
Arguments:
- electric: float32 [3, 64, 128, 256], P(None, 'gx', 'gy'), may hold values from -6 to 6
- magnetic: float32 [3, 64, 128, 256], P(None, 'gx', 'gy'), may hold values from -6 to 6
- aux_electric: float32 [6, 64, 128, 256], P(None, 'gx', 'gy'), may hold values from -3 to 3
- aux_magnetic: float32 [6, 64, 128, 256], P(None, 'gx', 'gy'), may hold values from -3 to 3
- grades: int32 [3, 64, 128, 256], P(None, 'gx', 'gy'), may hold values from 0 to 3
- permittivity: float32 [64, 128, 256], P('gx', 'gy'), may hold values from 1 to 8
- dipole_cell: int32 [3, 16384], P(None, ('gx', 'gy')), may hold values from 0 to 255, as said below
- dipole_port: int32 [16384], P(('gx', 'gy')), may hold values from 0 to 511
- live_count: int32 [32], P(('gx', 'gy')), may hold values from 1 to 512, as said below
- injection: bfloat16 [16384, 512], P(('gx', 'gy')), may hold values from -0.25 to 0.25
- waveform: bfloat16 [512, 16], replicated, may hold values from -6 to 6
Outputs:
- electric_out: float32 [3, 64, 128, 256], P(None, 'gx', 'gy')
- magnetic_out: float32 [3, 64, 128, 256], P(None, 'gx', 'gy')
- port_power: float32 [16, 512], replicated
The draws below stay inside these ranges and needn't reach their ends.
Inputs may be any that keep to these rules, and one draw needn't show every extreme that they name: `dipole_cell`: slot s lies in the block of cells held by the device that holds slot s. The live slots of a device are its first live_count ones; some device has all 512 live.
All inputs are finite; a program needn't handle non-finite values.
Results may differ from the reference program's by a relative error of at most 0.0003.
Values sent between devices are 32-bit elements; how exact they have to be, the bound alone decides.
No kernel may reach another device: no remote copies, remote signals or barrier semaphores. Data moves between devices by JAX's collectives and lax.ppermute only.
A program may use at most 128 MiB of HBM per device.

```python
import math
import jax
import jax.numpy as jnp
from jax import lax

CX = 16
CY = 16
NZ = 256
DIP_DEV = 512
STEPS = 16
PORTS = 512
NX = 64
NY = 128
DIPOLES = 16384


def draw_dipole_cell(key, part):
    across = NY // CY
    slots = jnp.arange(DIPOLES, dtype=jnp.int32)
    owner = slots // DIP_DEV
    row_block = owner // across
    col_block = owner % across
    key_x, key_y, key_z = jax.random.split(jax.random.fold_in(key, 11), 3)
    coord_x = row_block * CX + jax.random.randint(key_x, (DIPOLES,), 0, CX)
    coord_y = col_block * CY + jax.random.randint(key_y, (DIPOLES,), 0, CY)
    coord_z = jax.random.randint(key_z, (DIPOLES,), 0, NZ)
    return jnp.stack([coord_x, coord_y, coord_z]).astype(jnp.int32)


def draw_dipole_port(key, part):
    devices = DIPOLES // DIP_DEV
    share = PORTS // devices
    slots = jnp.arange(DIPOLES, dtype=jnp.int32)
    owner = slots // DIP_DEV
    key_near, key_far, key_pick = jax.random.split(jax.random.fold_in(key, 23), 3)
    near = owner * share + jax.random.randint(key_near, (DIPOLES,), 0, share)
    far = jax.random.randint(key_far, (DIPOLES,), 0, PORTS)
    pick = jax.random.randint(key_pick, (DIPOLES,), 0, 4)
    return jnp.where(pick == 0, far, near).astype(jnp.int32)


def draw_live_count(key, part):
    devices = DIPOLES // DIP_DEV
    key_one, key_two, key_full = jax.random.split(jax.random.fold_in(key, 37), 3)
    first = jax.random.randint(key_one, (devices,), 1, DIP_DEV + 1)
    second = jax.random.randint(key_two, (devices,), 1, DIP_DEV + 1)
    counts = jnp.minimum(first, second)
    full = jax.random.randint(key_full, (), 0, devices)
    return jnp.where(jnp.arange(devices) == full, DIP_DEV, counts).astype(jnp.int32)


def place_ends(values, own_key, least, top_value):
    spot = [jax.random.randint(jax.random.fold_in(own_key, axis), (), 0, length) for axis, length in enumerate(values.shape)]
    main_axis = values.shape.index(max(values.shape))
    next_to = spot[:main_axis] + [(spot[main_axis] + 1) % values.shape[main_axis]] + spot[main_axis + 1:]
    return values.at[tuple(spot)].set(least).at[tuple(next_to)].set(top_value)


def block_levels(rng, extent, cuts, least, top_value):
    loudness = 1.0
    for dim, blocks in cuts:
        steps = jax.random.uniform(jax.random.fold_in(jax.random.fold_in(rng, 6), dim), (blocks,), jnp.float32, least / len(cuts), top_value / len(cuts))
        loudness = loudness * jnp.repeat(jnp.exp(steps), extent[dim] // blocks).reshape((-1,) + (1,) * (len(extent) - 1 - dim))
    return loudness


def normal_values(rng, shape, width, limit, cuts=(), kind=jnp.bfloat16):
    values = jax.random.normal(rng, shape, jnp.float32) * width
    if len(cuts) > 0:
        values = block_levels(rng, shape, cuts, -0.22, 0.18) * values
    return jnp.clip(values, min=-limit, max=limit).astype(kind)


def setup_inputs(seed: int = 0) -> dict:
    keys = jax.random.split(jax.random.key(seed), 12)
    electric = normal_values(keys[0], (3, NX, NY, NZ), 1.0, 6.0, ((1, 4), (2, 8)), jnp.float32)
    magnetic = normal_values(keys[1], (3, NX, NY, NZ), 1.0, 6.0, ((1, 4), (2, 8)), jnp.float32)
    aux_electric = normal_values(keys[2], (6, NX, NY, NZ), 0.4, 3.0, ((1, 4), (2, 8)), jnp.float32)
    aux_magnetic = normal_values(keys[3], (6, NX, NY, NZ), 0.4, 3.0, ((1, 4), (2, 8)), jnp.float32)
    grades = place_ends(jax.random.randint(keys[4], (3, NX, NY, NZ), 0, 4), jax.random.fold_in(keys[4], 1), 0, 3).astype(jnp.int32)
    permittivity = jnp.clip(jnp.exp(math.log(8.0) - 2.0794415 * jax.random.uniform(keys[5], (NX, NY, NZ), jnp.float32) ** block_levels(keys[5], (NX, NY, NZ), ((0, 4), (1, 8)), -0.2, 0.2)), 1.0, 8.0)
    dipole_cell = draw_dipole_cell(jax.random.fold_in(keys[11], 71), 0)
    dipole_port = draw_dipole_port(jax.random.fold_in(keys[11], 71), 0)
    live_count = draw_live_count(jax.random.fold_in(keys[11], 71), 0)
    injection = normal_values(keys[9], (DIPOLES, PORTS), PORTS ** -0.5, 0.25, ((0, 32),))
    waveform = normal_values(keys[10], (PORTS, STEPS), 1.0, 6.0)
    return dict(electric=electric, magnetic=magnetic, aux_electric=aux_electric, aux_magnetic=aux_magnetic, grades=grades, permittivity=permittivity, dipole_cell=dipole_cell, dipole_port=dipole_port, live_count=live_count, injection=injection, waveform=waveform)


courant = 0.55
absorb_keep = (0.0, 0.92, 0.75, 0.45)
absorb_take = (0.0, -0.06, -0.18, -0.35)
derivative_pairs = ((2, 1), (1, 2), (0, 2), (2, 0), (1, 0), (0, 1))


def difference(values, axis, plane, forward):
    length = values.shape[axis]
    if plane is None:
        shape = list(values.shape)
        shape[axis] = 1
        plane = jnp.zeros(shape, values.dtype)
    if forward:
        after = jnp.concatenate([lax.slice_in_dim(values, 1, length, axis=axis), plane], axis)
        return after - values
    before = jnp.concatenate([plane, lax.slice_in_dim(values, 0, length - 1, axis=axis)], axis)
    return values - before


def grade_table(grades, table):
    result = jnp.zeros(grades.shape, jnp.float32)
    for level in range(1, 4):
        result = result + jnp.where(grades == level, table[level], 0.0)
    return result


def curl(field, auxiliary, keep, take, planes, forward):
    terms = []
    updated = []
    for number, (component, axis) in enumerate(derivative_pairs):
        plane = None
        if planes is not None and axis == 0:
            plane = planes[0][component - 1]
        if planes is not None and axis == 1:
            plane = planes[1][component // 2]
        slope = difference(field[component], axis, plane, forward)
        carried = keep[axis] * auxiliary[number] + take[axis] * slope
        terms.append(slope + carried)
        updated.append(carried)
    rotation = jnp.stack([terms[0] - terms[1], terms[2] - terms[3], terms[4] - terms[5]])
    return rotation, jnp.stack(updated)


def reference(electric, magnetic, aux_electric, aux_magnetic, grades, permittivity, dipole_cell, dipole_port, live_count, injection, waveform):
    keep = grade_table(grades, absorb_keep)
    take = grade_table(grades, absorb_take)
    slots = jnp.arange(DIPOLES, dtype=jnp.int32)
    live = ((slots % DIP_DEV) < live_count[slots // DIP_DEV]).astype(jnp.float32)
    current = jnp.dot(injection, waveform, preferred_element_type=jnp.float32) * live[:, None]
    flat_cell = (dipole_cell[0] * (NY * NZ) + dipole_cell[1] * NZ + dipole_cell[2]).astype(jnp.int32)
    factor = courant / permittivity
    powers = []
    for step in range(STEPS):
        rotation, aux_electric = curl(electric, aux_electric, keep, take, None, True)
        magnetic = magnetic - courant * rotation
        rotation, aux_magnetic = curl(magnetic, aux_magnetic, keep, take, None, False)
        electric = electric + factor * rotation
        current_now = current[:, step]
        flat_z = electric[2].reshape(-1).at[flat_cell].add(-courant * current_now)
        drive = current_now * flat_z[flat_cell]
        electric = jnp.concatenate([electric[0:2], flat_z.reshape(1, NX, NY, NZ)], 0)
        powers.append(jax.ops.segment_sum(drive, dipole_port, PORTS))
    return electric, magnetic, jnp.stack(powers)
```

```python
import functools

import jax
import jax.numpy as jnp
from jax import lax
from jax.experimental import pallas as pl
from jax.experimental.pallas import tpu as pltpu
from jax.sharding import PartitionSpec as P

courant = 0.55
absorb_keep = (0.0, 0.92, 0.75, 0.45)
absorb_take = (0.0, -0.06, -0.18, -0.35)
pairs = ((2, 1), (1, 2), (0, 2), (2, 0), (1, 0), (0, 1))

vmem_spec = pl.BlockSpec(memory_space=pltpu.VMEM)


def passed_along(block, axis, distance):
    devices = range(lax.axis_size(axis))
    route = [(i - distance, i) for i in devices if i - distance in devices]
    return lax.ppermute(block, axis, route)


def grade_table(grades, table):
    result = jnp.zeros(grades.shape, jnp.float32)
    for level in range(1, 4):
        result = result + jnp.where(grades == level, table[level], 0.0)
    return result


def fixed(x):
    return pltpu.with_memory_space_constraint(x, pltpu.VMEM)


def call(body, args, pinned, outs, aliases, limit=6 << 20):
    args = [fixed(a) if i in pinned else a for i, a in enumerate(args)]
    shapes = [
        pltpu.VMEM(s, d) if keep else jax.ShapeDtypeStruct(s, d) for s, d, keep in outs
    ]
    return pl.pallas_call(
        body,
        out_shape=shapes,
        in_specs=[vmem_spec] * len(args),
        out_specs=[vmem_spec] * len(outs),
        input_output_aliases=aliases,
        compiler_params=pltpu.CompilerParams(vmem_limit_bytes=limit),
    )(*args)


def shifted(v, axis, forward, inner):
    n = v.shape[axis]
    rolled = pltpu.roll(v, n - 1 if forward else 1, axis)
    return jnp.where(inner, rolled, 0.0)


def main_kernel(forward, *refs):
    if forward:
        src, dst, mem, keep, take, dst_o, mem_o = refs
    else:
        src, dst, mem, keep, take, factor, source, dst_o, mem_o = refs
    _, nx, ny, nz = src.shape
    row = lax.broadcasted_iota(jnp.int32, (ny, nz), 0)
    col = lax.broadcasted_iota(jnp.int32, (ny, nz), 1)
    inner_y = row < ny - 1 if forward else row > 0
    inner_z = col < nz - 1 if forward else col > 0

    def plane(x, _):
        if forward:
            beside = jnp.minimum(x + 1, nx - 1)
            valid = (x < nx - 1).astype(jnp.float32)
        else:
            beside = jnp.maximum(x - 1, 0)
            valid = (x > 0).astype(jnp.float32)
        here = [src[c, x] for c in range(3)]
        kept = [keep[d, x] for d in range(3)]
        taken = [take[d, x] for d in range(3)]
        terms = []
        for k, (c, d) in enumerate(pairs):
            if d == 0:
                other = src[c, beside] * valid
            elif d == 1:
                other = shifted(here[c], 0, forward, inner_y)
            else:
                other = shifted(here[c], 1, forward, inner_z)
            slope = other - here[c] if forward else here[c] - other
            carried = kept[d] * mem[k, x] + taken[d] * slope
            mem_o[k, x] = carried
            terms.append(slope + carried)
        for c in range(3):
            rotation = terms[2 * c] - terms[2 * c + 1]
            if forward:
                dst_o[c, x] = dst[c, x] - courant * rotation
            else:
                value = dst[c, x] + factor[x] * rotation
                if c == 2:
                    value = value - source[x]
                dst_o[c, x] = value
        return 0

    lax.fori_loop(0, nx, plane, 0, unroll=2)


def edge_kernel(forward, *refs):
    if forward:
        dst, mem, take, px, py, dst_o, mem_o, sx, sy = refs
        weight = lambda x, ys: -courant
        sign = 1.0
    else:
        dst, mem, take, factor, px, py, dst_o, mem_o, sx, sy = refs
        weight = lambda x, ys: factor[x, ys]
        sign = -1.0
    _, nx, ny, nz = dst.shape
    x = nx - 1 if forward else 0
    whole = slice(None)
    taken = take[0, x]
    scale = weight(x, whole) * sign
    for k, p in ((3, 1), (4, 0)):
        part = taken * px[p]
        mem_o[k, x] = mem[k, x] + sign * part
        grown = scale * (px[p] + part)
        c = k // 2
        if k == 3:
            dst_o[c, x] = dst[c, x] - grown
        else:
            dst_o[c, x] = dst[c, x] + grown
    y = ny - 1 if forward else 0
    ys = slice(y, y + 1)
    for i in range(nx):
        taken = take[1, i, ys]
        scale = weight(i, ys) * sign
        for k, p in ((0, 1), (5, 0)):
            part = taken * py[p, i:i + 1]
            mem_o[k, i, ys] = mem[k, i, ys] + sign * part
            grown = scale * (py[p, i:i + 1] + part)
            c = k // 2
            base = dst_o if (k == 5 and i == x) else dst
            if k == 0:
                fresh = base[c, i, ys] + grown
            else:
                fresh = base[c, i, ys] - grown
            dst_o[c, i, ys] = fresh
            sy[c // 2, i:i + 1] = fresh
    sx[0] = dst_o[1, x]
    sx[1] = dst_o[2, x]


def halves(values):
    high = values.astype(jnp.bfloat16)
    return high, (values - high.astype(jnp.float32)).astype(jnp.bfloat16)


def source_of(cell_t, depth, pushed):
    high, low = halves(pushed)
    top = jnp.dot(cell_t * high, depth, preferred_element_type=jnp.float32)
    return top + jnp.dot(cell_t * low, depth, preferred_element_type=jnp.float32)


def dipole_kernel(step, last, *refs):
    refs = list(refs)
    first = step == 0
    if not first:
        field, cell = refs[0:2]
        refs = refs[2:]
    depth = refs[0]
    refs = refs[1:]
    if not last:
        cell_t, pushed = refs[0:2]
        refs = refs[2:]
    if not first:
        _, nx, ny, nz = field.shape
        values = field[2].reshape(nx * ny, nz)
        top, rest = halves(values)
        picked = jnp.dot(cell[...], top, preferred_element_type=jnp.float32)
        picked = picked + jnp.dot(cell[...], rest, preferred_element_type=jnp.float32)
        refs[0][...] = jnp.sum(picked * depth[...].astype(jnp.float32), axis=1, keepdims=True)
        refs = refs[1:]
    if not last:
        out = refs[0]
        out[...] = source_of(cell_t[...], depth[...], pushed[step:step + 1]).reshape(out.shape)


def summed(values, axis):
    size = lax.axis_size(axis)
    if size & (size - 1):
        return lax.psum(values, axis)
    distance = 1
    while distance < size:
        values = values + lax.ppermute(values, axis, [(i, i ^ distance) for i in range(size)])
        distance *= 2
    return values


def local(
    electric,
    magnetic,
    aux_electric,
    aux_magnetic,
    grades,
    permittivity,
    dipole_cell,
    dipole_port,
    live_count,
    injection,
    waveform,
):
    nx, ny, nz = electric.shape[1:]
    slots = dipole_cell.shape[1]
    ports, steps = waveform.shape
    f32 = jnp.float32
    row_index = lax.axis_index("gx")
    col_index = lax.axis_index("gy")
    plane_cell = (dipole_cell[0] - row_index * nx) * ny + (dipole_cell[1] - col_index * ny)
    cells = jnp.arange(nx * ny, dtype=jnp.int32)
    cell = (plane_cell[:, None] == cells[None, :]).astype(jnp.bfloat16)
    cell_t = (cells[:, None] == plane_cell[None, :]).astype(jnp.bfloat16)
    depth = (dipole_cell[2][:, None] == jnp.arange(nz, dtype=jnp.int32)[None, :]).astype(
        jnp.bfloat16
    )
    live = (jnp.arange(slots, dtype=jnp.int32) < live_count[0]).astype(f32)
    current = jnp.dot(injection, waveform, preferred_element_type=f32) * live[:, None]
    pushed = courant * current.T
    members = (dipole_port[:, None] == jnp.arange(ports, dtype=jnp.int32)[None, :]).astype(f32)
    factor = courant / permittivity
    keep = grade_table(grades, absorb_keep)
    take = grade_table(grades, absorb_take)

    field = (3, nx, ny, nz)
    memory = (6, nx, ny, nz)
    block = (nx, ny, nz)
    send_x = ((2, ny, nz), f32, False)
    send_y = ((2, nx, nz), f32, False)
    state = [(field, f32, True), (memory, f32, True)]
    picks = []
    (source,) = call(
        functools.partial(dipole_kernel, 0, False),
        [depth, cell_t, pushed],
        range(3),
        [(block, f32, True)],
        {},
    )
    sx = jnp.stack([electric[1, 0], electric[2, 0]])
    sy = jnp.stack([electric[0, :, 0], electric[2, :, 0]])
    for step in range(steps):
        px = passed_along(sx, "gx", -1)
        py = passed_along(sy, "gy", -1)
        magnetic, aux_electric = call(
            functools.partial(main_kernel, True),
            [electric, magnetic, aux_electric, keep, take],
            range(5),
            state,
            {1: 0, 2: 1},
        )
        magnetic, aux_electric, sx, sy = call(
            functools.partial(edge_kernel, True),
            [magnetic, aux_electric, take, px, py],
            range(3),
            state + [send_x, send_y],
            {0: 0, 1: 1},
        )
        px = passed_along(sx, "gx", 1)
        py = passed_along(sy, "gy", 1)
        electric, aux_magnetic = call(
            functools.partial(main_kernel, False),
            [magnetic, electric, aux_magnetic, keep, take, factor, source],
            range(7),
            state,
            {1: 0, 2: 1},
        )
        electric, aux_magnetic, sx, sy = call(
            functools.partial(edge_kernel, False),
            [electric, aux_magnetic, take, factor, px, py],
            range(4),
            state + [send_x, send_y],
            {0: 0, 1: 1},
        )
        last = step == steps - 1
        args = [electric, cell, depth]
        outs = [((slots, 1), f32, False)]
        if not last:
            args += [cell_t, pushed]
            outs.append((block, f32, True))
        results = call(
            functools.partial(dipole_kernel, step + 1, last), args, range(len(args)), outs, {}
        )
        picks.append(results[0])
        if not last:
            source = results[1]
    record = jnp.concatenate(picks, axis=1) * current
    partial_value = lax.dot_general(
        record, members, (((0,), (0,)), ((), ())), precision=lax.Precision.HIGHEST
    )
    port_power = summed(summed(partial_value, "gx"), "gy")
    return (electric, magnetic, port_power)


def solution(mesh):
    in_specs = (
        P(None, "gx", "gy", None),
        P(None, "gx", "gy", None),
        P(None, "gx", "gy", None),
        P(None, "gx", "gy", None),
        P(None, "gx", "gy", None),
        P("gx", "gy", None),
        P(None, ("gx", "gy")),
        P(("gx", "gy")),
        P(("gx", "gy")),
        P(("gx", "gy"), None),
        P(),
    )
    out_specs = (P(None, "gx", "gy", None), P(None, "gx", "gy", None), P())
    return jax.shard_map(local, mesh=mesh, in_specs=in_specs, out_specs=out_specs, check_vma=False)
```
